512 devices in a mesh: section: 64 (over y_hi, z, core), mp: 8 (over y_lo, x).
Axes of the slice: x: 4, y: 4 (y_hi: 2, y_lo: 2; y = y_hi * 2 + y_lo), z: 16, core: 2. Of those that a mesh axis runs over, the one named last changes fastest.
Arguments:
- gate_weight: bfloat16 [2, 2048, 5632], P(None, 'section', 'mp'), may hold values from -6 to 6
- up_weight: bfloat16 [2, 2048, 5632], P(None, 'section', 'mp'), may hold values from -6 to 6
- hidden_map: int32 [2048], replicated, may hold values from 0 to 2047, as said below
- ffn_map: int32 [5376], replicated, may hold values from 0 to 5631, as said below
Outputs:
- grown_gate: bfloat16 [2, 2, 2048, 11008], P(None, None, 'section', 'mp')
- grown_up: bfloat16 [2, 2, 2048, 11008], P(None, None, 'section', 'mp')
The draws below stay inside these ranges and needn't reach their ends.
Inputs may be any that keep to these rules, and one draw needn't show every extreme that they name: `hidden_map`: entry i names the old unit copied by new unit 2048 + i. Within each aligned block of 32 entries, at most 1 entries name units of any one block of 32 old units, and some block of old units is named exactly 1 times. `ffn_map`: entry j names the FFN unit of the next layer copied by added unit j % 672 of FFN block j // 672. Within each aligned block of 672 entries, at most 84 entries name units of any one block of 704 old FFN units, and in each aligned block some block of old units is named exactly 84 times.
All inputs are finite; a program needn't handle non-finite values.
Results may differ from the reference program's by a relative error of at most 0.001.
Values may be sent and summed in bfloat16 or wider, within the bound.
A program may use at most 64 MiB of HBM per device.

```python
import jax
import jax.numpy as jnp

D_OLD = 2048
FF_OLD = 5632
LAYERS = 2
FF_EXTRA = 5376
NARROW = 704
EXTRA_DEV = 672
SHARD_ROWS = 32
BLOCKS = 64
N_MP = 8


def draw_hidden_map(key, part):
    owners = jax.vmap(lambda single: jax.random.permutation(single, BLOCKS))(jax.random.split(jax.random.fold_in(key, 7), BLOCKS))
    slots = jnp.arange(SHARD_ROWS) % BLOCKS
    chosen = owners[:, slots]
    within = jax.random.randint(jax.random.fold_in(key, 8), (BLOCKS, SHARD_ROWS), 0, SHARD_ROWS)
    return (chosen * SHARD_ROWS + within).reshape(-1).astype(jnp.int32)


def draw_ffn_map(key, part):
    splits = FF_EXTRA // EXTRA_DEV
    owners = jax.vmap(lambda single: jax.random.permutation(single, splits))(jax.random.split(jax.random.fold_in(key, 5), splits))
    slots = jnp.arange(EXTRA_DEV) % splits
    chosen = owners[:, slots]
    within = jax.random.randint(jax.random.fold_in(key, 6), (splits, EXTRA_DEV), 0, NARROW)
    return (chosen * NARROW + within).reshape(-1).astype(jnp.int32)


def shard_levels(own_key, extent, shards, low, largest):
    def one(axis_at, blocks):
        draws = jax.random.uniform(jax.random.fold_in(jax.random.fold_in(own_key, 6), axis_at), (blocks,), jnp.float32, low / len(shards), largest / len(shards))
        return jnp.repeat(jnp.exp(draws), extent[axis_at] // blocks).reshape((-1,) + (1,) * (len(extent) - axis_at - 1))

    factor_of = one(*shards[0])
    for cut in shards[1:]:
        factor_of = factor_of * one(*cut)
    return factor_of


def scatter_about(stream_key, dims, deviation, limit, cuts=(), kind=jnp.bfloat16):
    array = deviation * jax.random.normal(stream_key, dims, jnp.float32)
    if cuts:
        array = array * shard_levels(stream_key, dims, cuts, -0.22, 0.18)
    return jnp.clip(array, -limit, limit).astype(kind)


def setup_inputs(seed: int = 0) -> dict:
    arg_keys = jax.random.split(jax.random.key(seed), 5)
    return {
        "gate_weight": scatter_about(arg_keys[0], (LAYERS, D_OLD, FF_OLD), 1.0, 6.0, ((1, 64), (2, 8))),
        "up_weight": scatter_about(arg_keys[1], (LAYERS, D_OLD, FF_OLD), 1.0, 6.0, ((1, 64), (2, 8))),
        "hidden_map": draw_hidden_map(jax.random.fold_in(arg_keys[4], 71), 0),
        "ffn_map": draw_ffn_map(jax.random.fold_in(arg_keys[4], 71), 0),
    }


def reference(gate_weight, up_weight, hidden_map, ffn_map):
    layers, d_old, ff_old = gate_weight.shape
    narrow = ff_old // N_MP
    extra_dev = ffn_map.shape[0] // N_MP
    counts = jax.ops.segment_sum(jnp.ones((d_old,), jnp.float32), hidden_map.astype(jnp.int32), num_segments=d_old) + 1.0
    sources = jnp.concatenate([jnp.arange(d_old, dtype=jnp.int32), hidden_map.astype(jnp.int32)])
    divisor = counts[sources].reshape(2, d_old)
    next_layer = jnp.minimum(jnp.arange(layers, dtype=jnp.int32) + 1, layers - 1)

    def widen_matrix(weight):
        rows_taken = jnp.take(weight, sources, axis=1).reshape(layers, 2, d_old, ff_old)
        added = jnp.take(rows_taken[next_layer], ffn_map.astype(jnp.int32), axis=3)
        base_part = rows_taken.reshape(layers, 2, d_old, N_MP, narrow)
        added_part = added.reshape(layers, 2, d_old, N_MP, extra_dev)
        widened = jnp.concatenate([base_part, added_part], axis=4).reshape(layers, 2, d_old, N_MP * (narrow + extra_dev))
        return (widened.astype(jnp.float32) / divisor[None, :, :, None]).astype(jnp.bfloat16)

    return widen_matrix(gate_weight), widen_matrix(up_weight)
```

```python
import jax
import jax.numpy as jnp
from jax import lax
from jax.experimental import pallas as pl
from jax.experimental.pallas import tpu as pltpu
from jax.sharding import PartitionSpec as P

MESH = pl.DeviceIdType.MESH
BF16, F32, I32 = jnp.bfloat16, jnp.float32, jnp.int32
LANES = 128


def lane_iota(shape):
    return lax.broadcasted_iota(I32, shape, len(shape) - 1)


def row_iota(shape):
    return lax.broadcasted_iota(I32, shape, len(shape) - 2)


def ranks(hit, wide):
    upper = row_iota((LANES, LANES)) < lane_iota((LANES, LANES))
    steps = jnp.concatenate([upper.astype(F32), jnp.ones((LANES, LANES), F32)], axis=1).astype(BF16)
    flags = hit.astype(F32).astype(BF16)
    carry = jnp.zeros((hit.shape[0], LANES), F32)
    pieces = []
    for t in range(wide // LANES):
        both = jnp.dot(flags[:, t * LANES : (t + 1) * LANES], steps, preferred_element_type=F32)
        pieces.append(both[:, :LANES] + carry)
        carry = carry + both[:, LANES:]
    return jnp.concatenate(pieces, axis=1).astype(I32)


def solution(mesh):
    blocks, splits = mesh.shape["section"], mesh.shape["mp"]

    def local(gate_weight, up_weight, hidden_map, ffn_map):
        layers, rows, narrow = gate_weight.shape
        extra = ffn_map.shape[0] // splits
        wide = narrow + extra
        cap = extra // splits
        slots = -(-cap // 32) * 32
        main = narrow // LANES * LANES
        tail = narrow - main
        lead = main + LANES
        spread = -(-(wide - main) // LANES) * LANES
        hrows = hidden_map.shape[0] // LANES
        frows = ffn_map.shape[0] // LANES
        per_row = LANES // rows
        z_chips = blocks // 4

        def kernel(gate_h, up_h, hmap_h, fmap_h, out_g, out_u, gv, uv, hm, fm, own1, own0, send1, recv1, send0, recv0,
                   xs, fr, colpick, place, bsend, brecv, stage, in_sem, s1, r1, s0, r0, sb, rb, out_sem):
            me = lax.axis_index("section")
            col = lax.axis_index("mp")
            half, z, core = me // (2 * z_chips), (me // 2) % z_chips, me % 2

            def peer(i):
                n = i // 4
                step = (n + 1) // 2
                dz = z_chips // 2 + jnp.where(n % 2 == 1, -step, step)
                other = 3 - i % 4
                return ((half + other // 2) % 2) * (2 * z_chips) + ((z + dz) % z_chips) * 2 + (core + other % 2) % 2

            barrier = pltpu.get_barrier_semaphore()

            @pl.loop(0, blocks - 1)
            def _(i):
                pl.semaphore_signal(barrier, 1, device_id={"section": peer(i)}, device_id_type=MESH)

            for k in range(1, splits):
                pl.semaphore_signal(barrier, 1, device_id={"mp": (col + k) % splits}, device_id_type=MESH)

            loads = [
                pltpu.make_async_copy(src, dst, in_sem.at[n])
                for n, (src, dst) in enumerate(((hmap_h, hm), (gate_h, gv), (up_h, uv), (fmap_h, fm)))
            ]
            for copy in loads:
                copy.start()

            loads[0].wait()
            spread_map = jnp.concatenate([jnp.broadcast_to(hm[r : r + 1, :], (2 * per_row, LANES)) for r in range(hrows)], axis=0)
            shape = (2 * blocks, LANES)
            within = spread_map - me * rows
            mine = (within >= 0) & (within < rows) & (lane_iota(shape) // rows == (row_iota(shape) // 2) % per_row)
            chosen = jnp.sum(jnp.where(mine, within + 1, 0), axis=1, keepdims=True) - 1
            side = row_iota((2 * blocks, 1)) % 2
            target = jnp.where(chosen >= 0, chosen + side * rows, -1)
            pick_rows = (target == lane_iota((2 * blocks, 2 * rows))).astype(F32).astype(BF16)

            used = jnp.zeros((rows, LANES), F32)
            for r in range(hrows):
                entry = jnp.broadcast_to(hm[r : r + 1, :], (rows, LANES))
                used = used + (entry == me * rows + row_iota((rows, LANES))).astype(F32)
            counts = jnp.sum(used, axis=1, keepdims=True) + 1.0
            counts = jnp.concatenate([counts, counts], axis=0)

            loads[1].wait()
            loads[2].wait()
            new = [
                (jnp.concatenate([gv[layer], uv[layer]], axis=0).astype(F32) / counts) for layer in range(2)
            ]
            own1[:, :main] = new[1][:, :main].astype(BF16)
            own1[:, main:] = jnp.concatenate([new[1][:, main:], new[0][:, main:]], axis=1).astype(BF16)
            own0[...] = new[0][:, :main].astype(BF16)
            send1[...] = jnp.dot(pick_rows, own1[...], preferred_element_type=F32).astype(BF16).reshape(send1.shape)
            send0[...] = jnp.dot(pick_rows, own0[...], preferred_element_type=F32).astype(BF16).reshape(send0.shape)

            pl.semaphore_wait(barrier, blocks + splits - 2)

            for src, dst, ss, rs in ((send1, recv1, s1, r1), (send0, recv0, s0, r0)):

                @pl.loop(0, blocks - 1)
                def _(i, src=src, dst=dst, ss=ss, rs=rs):
                    to = peer(i)
                    pltpu.make_async_remote_copy(
                        src.at[to], dst.at[me], ss, rs, device_id={"section": to}, device_id_type=MESH
                    ).start()

            recv1[me] = send1[me]
            recv0[me] = send0[me]

            entry = jnp.broadcast_to(hm[pl.ds(me // per_row, 1), :], (rows, LANES))
            place_of = lane_iota((rows, LANES)) == (me % per_row) * rows + row_iota((rows, LANES))
            owner = jnp.sum(jnp.where(place_of, entry, 0), axis=1, keepdims=True) // rows
            landing = jnp.concatenate([2 * owner, 2 * owner + 1], axis=0)
            arrive = (landing == lane_iota((2 * rows, 2 * blocks))).astype(F32).astype(BF16)

            loads[3].wait()
            padded = -(-extra // LANES) * LANES
            for m in range(splits):
                first, shift = m * extra // LANES, m * extra % LANES
                n_rows = min(padded // LANES + 1, frows - first)
                flat = jnp.concatenate([fm[first + r : first + r + 1, :] for r in range(n_rows)], axis=1)
                flat = flat[:, shift : shift + extra]
                fr[m : m + 1, :extra] = flat
            fr[:, extra:] = jnp.full((splits, fr.shape[1] - extra), -1, I32)

            named = fr[...]
            within = named - col * narrow
            hit = (within >= 0) & (within < narrow)
            rank = jnp.where(hit, ranks(hit, padded), -1)
            for m in range(splits):
                taken = rank[m : m + 1, :] == row_iota((slots, padded))
                column = jnp.sum(jnp.where(taken, within[m : m + 1, :] + 1, 0), axis=1, keepdims=True) - 1
                colpick[m * slots : (m + 1) * slots, :] = (column == lane_iota((slots, narrow))).astype(F32).astype(BF16)

            wanted = jnp.broadcast_to(fr[pl.ds(col, 1), :], (splits, padded)) - row_iota((splits, padded)) * narrow
            hit = (wanted >= 0) & (wanted < narrow)
            code = jnp.where(hit, ranks(hit, padded) + row_iota((splits, padded)) * slots + 1, 0)
            code = jnp.sum(code, axis=0, keepdims=True) - 1
            code = jnp.concatenate([jnp.full((1, tail), -1, I32), code[:, : spread - tail]], axis=1)
            place[...] = (code == row_iota((splits * slots, spread))).astype(F32).astype(BF16)

            pltpu.make_async_copy(send1.at[pl.ds(0, blocks - 1)], recv1.at[pl.ds(0, blocks - 1)], r1).wait()
            got1 = jnp.dot(arrive, recv1[...].reshape(2 * blocks, lead), preferred_element_type=F32).astype(BF16)
            for w in range(2):
                a, b = w * rows, (w + 1) * rows
                xs[2 * a : 2 * a + rows, :] = own1[a:b, :]
                xs[2 * a + rows : 2 * b, :] = got1[a:b, :]
            bsend[...] = (
                lax.dot_general(colpick[...], xs[:, :narrow], (((1,), (1,)), ((), ())), preferred_element_type=F32)
                .astype(BF16)
                .reshape(bsend.shape)
            )
            for k in range(1, splits):
                to = (col + k) % splits
                pltpu.make_async_remote_copy(
                    bsend.at[to], brecv.at[col], sb, rb, device_id={"mp": to}, device_id_type=MESH
                ).start()
            brecv[col] = bsend[col]

            last = xs[:, main:].astype(F32)
            first_half = lane_iota((4 * rows, LANES)) < tail
            pads = [jnp.zeros((4 * rows, spread - LANES), F32)]
            ends = [jnp.where(first_half, end, 0.0) for end in (pltpu.roll(last, LANES - tail, 1), last)]
            for w in range(2):
                for k in range(2):
                    a = (2 * w + k) * rows
                    stage[w, 1, k, :, :main] = xs[a : a + rows, :main]
                stage[w, 0, 0, :, :main] = own0[w * rows : (w + 1) * rows, :]

            pltpu.make_async_copy(bsend.at[pl.ds(0, splits - 1)], brecv.at[pl.ds(0, splits - 1)], rb).wait()
            added = lax.dot_general(
                brecv[...].reshape(splits * slots, 4 * rows), place[...], (((0,), (0,)), ((), ())), preferred_element_type=F32
            )
            for layer in range(2):
                full = (added + jnp.concatenate([ends[layer]] + pads, axis=1)).astype(BF16)
                for w in range(2):
                    for k in range(2):
                        a = (2 * w + k) * rows
                        stage[w, layer, k, :, main:] = full[a : a + rows, : wide - main]
            outs = (out_g, out_u)
            writes = []
            for w in range(2):
                writes.append(pltpu.make_async_copy(stage.at[w, 1], outs[w].at[1], out_sem.at[3 * w]))
                writes.append(pltpu.make_async_copy(stage.at[w, 0, 0], outs[w].at[0, 0], out_sem.at[3 * w + 1]))
            for copy in writes:
                copy.start()

            pltpu.make_async_copy(send0.at[pl.ds(0, blocks - 1)], recv0.at[pl.ds(0, blocks - 1)], r0).wait()
            got0 = jnp.dot(arrive, recv0[...].reshape(2 * blocks, main), preferred_element_type=F32).astype(BF16)
            for w in range(2):
                stage[w, 0, 1, :, :main] = got0[w * rows : (w + 1) * rows, :]
                copy = pltpu.make_async_copy(stage.at[w, 0, 1], outs[w].at[0, 1], out_sem.at[3 * w + 2])
                copy.start()
                writes.append(copy)
            pltpu.make_async_copy(send1.at[pl.ds(0, blocks - 1)], recv1.at[pl.ds(0, blocks - 1)], s1).wait()
            pltpu.make_async_copy(send0.at[pl.ds(0, blocks - 1)], recv0.at[pl.ds(0, blocks - 1)], s0).wait()
            pltpu.make_async_copy(bsend.at[pl.ds(0, splits - 1)], brecv.at[pl.ds(0, splits - 1)], sb).wait()
            for copy in writes:
                copy.wait()

        padded = -(-extra // LANES) * LANES
        out = jax.ShapeDtypeStruct((layers, 2, rows, wide), BF16)
        anywhere = pl.BlockSpec(memory_space=pl.ANY)
        return pl.pallas_call(
            kernel,
            out_shape=(out, out),
            in_specs=[anywhere] * 4,
            out_specs=(anywhere, anywhere),
            scratch_shapes=[
                pltpu.VMEM(gate_weight.shape, BF16),
                pltpu.VMEM(gate_weight.shape, BF16),
                pltpu.VMEM((hrows, LANES), I32),
                pltpu.VMEM((frows, LANES), I32),
                pltpu.VMEM((2 * rows, lead), BF16),
                pltpu.VMEM((2 * rows, main), BF16),
                pltpu.VMEM((blocks, 2, lead), BF16),
                pltpu.VMEM((blocks, 2, lead), BF16),
                pltpu.VMEM((blocks, 2, main), BF16),
                pltpu.VMEM((blocks, 2, main), BF16),
                pltpu.VMEM((4 * rows, lead), BF16),
                pltpu.VMEM((splits, padded), I32),
                pltpu.VMEM((splits * slots, narrow), BF16),
                pltpu.VMEM((splits * slots, spread), BF16),
                pltpu.VMEM((splits, slots, 4 * rows), BF16),
                pltpu.VMEM((splits, slots, 4 * rows), BF16),
                pltpu.VMEM((2, layers, 2, rows, wide), BF16),
                pltpu.SemaphoreType.DMA((4,)),
                pltpu.SemaphoreType.DMA,
                pltpu.SemaphoreType.DMA,
                pltpu.SemaphoreType.DMA,
                pltpu.SemaphoreType.DMA,
                pltpu.SemaphoreType.DMA,
                pltpu.SemaphoreType.DMA,
                pltpu.SemaphoreType.DMA((6,)),
            ],
            compiler_params=pltpu.CompilerParams(collective_id=0, has_side_effects=True),
            name="grow",
        )(gate_weight, up_weight, hidden_map.reshape(hrows, LANES), ffn_map.reshape(frows, LANES))

    weights = P(None, "section", "mp")
    out_specs = (P(None, None, "section", "mp"),) * 2
    return jax.shard_map(local, mesh=mesh, in_specs=(weights, weights, P(), P()), out_specs=out_specs, check_vma=False)
```

```python
import functools

import jax
import jax.numpy as jnp
from jax import lax
from jax.experimental import pallas as pl
from jax.experimental.pallas import tpu as pltpu
from jax.sharding import PartitionSpec as P

MESH = pl.DeviceIdType.MESH
BF16, F32, I32 = jnp.bfloat16, jnp.float32, jnp.int32
LANES = 128


def lane_iota(shape):
    return lax.broadcasted_iota(I32, shape, len(shape) - 1)


def row_iota(shape):
    return lax.broadcasted_iota(I32, shape, len(shape) - 2)


def one_hot(hit):
    return hit.astype(F32).astype(BF16)


def ranks(hit, wide):
    upper = row_iota((LANES, LANES)) < lane_iota((LANES, LANES))
    steps = jnp.concatenate([upper.astype(F32), jnp.ones((LANES, LANES), F32)], axis=1).astype(BF16)
    flags = one_hot(hit)
    carry = jnp.zeros((hit.shape[0], LANES), F32)
    pieces = []
    for t in range(wide // LANES):
        both = jnp.dot(flags[:, t * LANES : (t + 1) * LANES], steps, preferred_element_type=F32)
        pieces.append(both[:, :LANES] + carry)
        carry = carry + both[:, LANES:]
    return jnp.concatenate(pieces, axis=1).astype(I32)


def write_out(gate_v, up_v, gate_h, up_h, sems):
    copies = [
        pltpu.make_async_copy(src.at[layer], dst.at[layer], sems.at[2 * n + layer])
        for n, (src, dst) in enumerate(((gate_v, gate_h), (up_v, up_h)))
        for layer in range(2)
    ]
    for copy in copies:
        copy.start()
    for copy in copies:
        copy.wait()


def solution(mesh):
    blocks, splits = mesh.shape["section"], mesh.shape["mp"]
    z_chips = blocks // 4
    reach = z_chips // 4

    def steps(first, last):
        order = [d for n in range(last, first - 1, -1) for d in ((n, z_chips - n) if 0 < n < z_chips // 2 else (n,))]
        return [(d, q) for d in order for q in range(4) if d or q]

    near = steps(0, reach)
    n_far = z_chips - 2 * reach - 1

    def local(gate_weight, up_weight, hidden_map, ffn_map):
        layers, rows, narrow = gate_weight.shape
        extra = ffn_map.shape[0] // splits
        wide = narrow + extra
        cap = extra // splits
        filled = -(-cap // 32) * 32
        main = narrow // LANES * LANES
        tail = narrow - main
        lead = main + LANES
        padded = -(-extra // LANES) * LANES
        spread = -(-(wide - main) // LANES) * LANES
        hrows = hidden_map.shape[0] // LANES
        frows = ffn_map.shape[0] // LANES
        per_row = LANES // rows
        cols = splits * LANES

        def kernel(gate_h, up_h, hmap_h, fmap_h, out_g, out_u, gv, uv, hm, fm, own1, own0, send1, recv1, send0, recv0,
                   got, fr, colpick, place, bsend, brecv, in_sem, s1, r1, s0, r0, sb, rb, ready):
            outs = (out_g, out_u)
            me = lax.axis_index("section")
            col = lax.axis_index("mp")
            half, z, core = me // (2 * z_chips), (me // 2) % z_chips, me % 2
            ring = [2 * z] + [2 * jnp.where(z + d >= z_chips, z + d - z_chips, z + d) for d in range(1, z_chips)]
            seat = [h * (2 * z_chips) + c for h in (half, 1 - half) for c in (core, 1 - core)]
            fellow = [jnp.where(col + k >= splits, col + k - splits, col + k) for k in range(splits)]

            barrier = pltpu.get_barrier_semaphore()
            for d, q in near:
                pl.semaphore_signal(barrier, 1, device_id={"section": seat[q] + ring[d]}, device_id_type=MESH)
            for to in fellow[1:]:
                pl.semaphore_signal(barrier, 1, device_id={"mp": to}, device_id_type=MESH)

            loads = [
                pltpu.make_async_copy(src, dst, in_sem.at[n])
                for n, (src, dst) in enumerate(((hmap_h, hm), (gate_h, gv), (up_h, uv), (fmap_h, fm)))
            ]
            for copy in loads:
                copy.start()

            loads[0].wait()
            spread_map = jnp.concatenate([jnp.broadcast_to(hm[r : r + 1, :], (2 * per_row, LANES)) for r in range(hrows)], axis=0)
            shape = (2 * blocks, LANES)
            within = spread_map - me * rows
            mine = (within >= 0) & (within < rows) & (lane_iota(shape) // rows == (row_iota(shape) // 2) % per_row)
            chosen = jnp.sum(jnp.where(mine, within + 1, 0), axis=1, keepdims=True) - 1
            side = row_iota((2 * blocks, 1)) % 2
            target = jnp.where(chosen >= 0, chosen + side * rows, -1)
            pick_rows = one_hot(target == lane_iota((2 * blocks, 2 * rows)))

            used = jnp.zeros((rows, LANES), F32)
            for r in range(hrows):
                entry = jnp.broadcast_to(hm[r : r + 1, :], (rows, LANES))
                used = used + (entry == me * rows + row_iota((rows, LANES))).astype(F32)
            counts = jnp.sum(used, axis=1, keepdims=True) + 1.0
            counts = jnp.concatenate([counts, counts], axis=0)

            loads[1].wait()
            loads[2].wait()
            new = [(jnp.concatenate([gv[layer], uv[layer]], axis=0).astype(F32) / counts) for layer in range(2)]
            own1[:, :main] = new[1][:, :main].astype(BF16)
            own1[:, main:] = jnp.concatenate([new[1][:, main:], new[0][:, main:]], axis=1).astype(BF16)
            own0[...] = new[0][:, :main].astype(BF16)
            send1[...] = jnp.dot(pick_rows, own1[...], preferred_element_type=F32).astype(BF16).reshape(send1.shape)
            send0[...] = jnp.dot(pick_rows, own0[...], preferred_element_type=F32).astype(BF16).reshape(send0.shape)
            recv1[me] = send1[me]
            recv0[me] = send0[me]

            pl.semaphore_wait(barrier, len(near) + splits - 1)
            for d in (reach, z_chips - reach):
                pl.semaphore_signal(ready, 1, device_id={"section": seat[0] + ring[d]}, device_id_type=MESH)

            def send(layer, to):
                src, dst, ss, rs = ((send0, recv0, s0, r0), (send1, recv1, s1, r1))[layer]
                pltpu.make_async_remote_copy(
                    src.at[to], dst.at[me], ss, rs, device_id={"section": to}, device_id_type=MESH
                ).start()

            for d, q in near:
                send(1, seat[q] + ring[d])

            loads[3].wait()
            for m in range(splits):
                first, shift = m * extra // LANES, m * extra % LANES
                n_rows = min(padded // LANES + 1, frows - first)
                flat = jnp.concatenate([fm[first + r : first + r + 1, :] for r in range(n_rows)], axis=1)
                fr[m : m + 1, :extra] = flat[:, shift : shift + extra]
            fr[:, extra:] = jnp.full((splits, padded - extra), -1, I32)

            within = fr[...] - col * narrow
            hit = (within >= 0) & (within < narrow)
            rank = jnp.where(hit, ranks(hit, padded), -1)
            for m in range(splits):
                taken = rank[m : m + 1, :] == row_iota((filled, padded))
                column = jnp.sum(jnp.where(taken, within[m : m + 1, :] + 1, 0), axis=1, keepdims=True) - 1
                colpick[m * LANES : m * LANES + filled, :] = one_hot(column == lane_iota((filled, narrow)))
                colpick[m * LANES + filled : (m + 1) * LANES, :] = jnp.zeros((LANES - filled, narrow), BF16)

            def exchange(part, values):
                chosen = lax.dot_general(values, colpick[...], (((1,), (1,)), ((), ())), preferred_element_type=F32).astype(BF16)
                for m in range(splits):
                    bsend[part, m] = chosen[:, m * LANES : (m + 1) * LANES]
                for to in fellow[1:]:
                    pltpu.make_async_remote_copy(
                        bsend.at[part, to], brecv.at[part, col], sb.at[part], rb.at[part], device_id={"mp": to}, device_id_type=MESH
                    ).start()
                brecv[part, col] = bsend[part, col]

            def arrived(buffers, sem):
                src, dst = buffers
                pltpu.make_async_copy(src.at[pl.ds(0, dst.shape[0] - 1)], dst.at[pl.ds(0, dst.shape[0] - 1)], sem).wait()

            def grow(part, last):
                arrived((bsend.at[part], brecv.at[part]), rb.at[part])
                added = jnp.zeros((2 * rows, spread), F32)
                for m in range(splits):
                    added += jnp.dot(brecv[part, m], place[m * LANES : (m + 1) * LANES, :], preferred_element_type=F32)
                first_half = lane_iota((2 * rows, LANES)) < tail
                for layer, end in enumerate((pltpu.roll(last, LANES - tail, 1), last)):
                    head = (added[:, :LANES] + jnp.where(first_half, end, 0.0)).astype(BF16)
                    for w in range(2):
                        a, b = w * rows, (w + 1) * rows
                        outs[w][layer, part, :, main:lead] = head[a:b, :]
                        outs[w][layer, part, :, lead:] = added[a:b, LANES : wide - main].astype(BF16)

            exchange(0, own1[:, :narrow])

            pl.semaphore_wait(ready, 2)
            turned = jnp.where((z + reach + 1 < z_chips) & (z + reach + n_far >= z_chips), z_chips - 1 - reach - z, 0)
            for i in range(n_far):
                ahead = jnp.where(i + turned >= n_far, i + turned - n_far, i + turned) + reach + 1 + z
                for q in range(4):
                    send(1, seat[q] + 2 * jnp.where(ahead >= z_chips, ahead - z_chips, ahead))

            wanted = jnp.broadcast_to(fr[pl.ds(col, 1), :], (splits, padded)) - row_iota((splits, padded)) * narrow
            hit = (wanted >= 0) & (wanted < narrow)
            code = jnp.where(hit, ranks(hit, padded) + row_iota((splits, padded)) * LANES + 1, 0)
            code = jnp.sum(code, axis=0, keepdims=True) - 1
            code = jnp.concatenate([jnp.full((1, tail), -1, I32), code[:, : spread - tail]], axis=1)
            place[...] = one_hot(code == row_iota((cols, spread)))

            entry = jnp.broadcast_to(hm[pl.ds(me // per_row, 1), :], (rows, LANES))
            place_of = lane_iota((rows, LANES)) == (me % per_row) * rows + row_iota((rows, LANES))
            owner = jnp.sum(jnp.where(place_of, entry, 0), axis=1, keepdims=True) // rows
            landing = jnp.concatenate([2 * owner, 2 * owner + 1], axis=0)
            arrive = one_hot(landing == lane_iota((2 * rows, 2 * blocks)))

            for w in range(2):
                a, b = w * rows, (w + 1) * rows
                outs[w][0, 0, :, :main] = own0[a:b, :]
                outs[w][1, 0, :, :main] = own1[a:b, :main]
            arrived((send1, recv1), s1)
            for j in range(z_chips):
                for q in range(1, 4):
                    send(0, seat[q] + 2 * j)
                pl.when(z != j)(functools.partial(send, 0, seat[0] + 2 * j))
            grow(0, own1[:, main:].astype(F32))

            arrived((send1, recv1), r1)
            got[...] = jnp.dot(arrive, recv1[...].reshape(2 * blocks, lead), preferred_element_type=F32).astype(BF16)
            exchange(1, got[:, :narrow])
            for w in range(2):
                outs[w][1, 1, :, :main] = got[w * rows : (w + 1) * rows, :main]
            arrived((send0, recv0), r0)
            got0 = jnp.dot(arrive, recv0[...].reshape(2 * blocks, main), preferred_element_type=F32).astype(BF16)
            for w in range(2):
                outs[w][0, 1, :, :main] = got0[w * rows : (w + 1) * rows, :]
            grow(1, got[:, main:].astype(F32))

            arrived((send0, recv0), s0)
            for part in range(2):
                arrived((bsend.at[part], brecv.at[part]), sb.at[part])

        out = jax.ShapeDtypeStruct((layers, 2, rows, wide), BF16)
        anywhere = pl.BlockSpec(memory_space=pl.ANY)
        inside = pl.BlockSpec(memory_space=pltpu.VMEM)
        both = (out, out)
        operands = (gate_weight, up_weight, hidden_map.reshape(hrows, LANES), ffn_map.reshape(frows, LANES))
        grown = pl.pallas_call(
            kernel,
            out_shape=both,
            in_specs=[pl.BlockSpec(memory_space=pltpu.HBM)] * 4,
            out_specs=(inside, inside),
            scratch_shapes=[
                pltpu.VMEM(gate_weight.shape, BF16),
                pltpu.VMEM(gate_weight.shape, BF16),
                pltpu.VMEM((hrows, LANES), I32),
                pltpu.VMEM((frows, LANES), I32),
                pltpu.VMEM((2 * rows, lead), BF16),
                pltpu.VMEM((2 * rows, main), BF16),
                pltpu.VMEM((blocks, 2, lead), BF16),
                pltpu.VMEM((blocks, 2, lead), BF16),
                pltpu.VMEM((blocks, 2, main), BF16),
                pltpu.VMEM((blocks, 2, main), BF16),
                pltpu.VMEM((2 * rows, lead), BF16),
                pltpu.VMEM((splits, padded), I32),
                pltpu.VMEM((cols, narrow), BF16),
                pltpu.VMEM((cols, spread), BF16),
                pltpu.VMEM((2, splits, 2 * rows, LANES), BF16),
                pltpu.VMEM((2, splits, 2 * rows, LANES), BF16),
                pltpu.SemaphoreType.DMA((4,)),
                pltpu.SemaphoreType.DMA,
                pltpu.SemaphoreType.DMA,
                pltpu.SemaphoreType.DMA,
                pltpu.SemaphoreType.DMA,
                pltpu.SemaphoreType.DMA((2,)),
                pltpu.SemaphoreType.DMA((2,)),
                pltpu.SemaphoreType.REGULAR,
            ],
            compiler_params=pltpu.CompilerParams(collective_id=0, has_side_effects=True, vmem_limit_bytes=24 << 20),
            name="grow",
        )(*(pltpu.with_memory_space_constraint(x, pltpu.HBM) for x in operands))
        return pl.pallas_call(
            write_out,
            out_shape=both,
            in_specs=[inside] * 2,
            out_specs=(anywhere, anywhere),
            scratch_shapes=[pltpu.SemaphoreType.DMA((4,))],
            compiler_params=pltpu.CompilerParams(vmem_limit_bytes=24 << 20),
            name="write",
        )(*grown)

    weights = P(None, "section", "mp")
    out_specs = (P(None, None, "section", "mp"),) * 2
    return jax.shard_map(local, mesh=mesh, in_specs=(weights, weights, P(), P()), out_specs=out_specs, check_vma=False)
```

```python
import functools

import jax
import jax.numpy as jnp
from jax import lax
from jax.experimental import pallas as pl
from jax.experimental.pallas import tpu as pltpu
from jax.sharding import PartitionSpec as P

MESH = pl.DeviceIdType.MESH
BF16, F32, I32 = jnp.bfloat16, jnp.float32, jnp.int32
LANES = 128


def lane_iota(shape):
    return lax.broadcasted_iota(I32, shape, len(shape) - 1)


def row_iota(shape):
    return lax.broadcasted_iota(I32, shape, len(shape) - 2)


def one_hot(hit):
    return hit.astype(F32).astype(BF16)


def ranks(hit, wide):
    upper = row_iota((LANES, LANES)) < lane_iota((LANES, LANES))
    steps = jnp.concatenate([upper.astype(F32), jnp.ones((LANES, LANES), F32)], axis=1).astype(BF16)
    flags = one_hot(hit)
    carry = jnp.zeros((hit.shape[0], LANES), F32)
    pieces = []
    for t in range(wide // LANES):
        both = jnp.dot(flags[:, t * LANES : (t + 1) * LANES], steps, preferred_element_type=F32)
        pieces.append(both[:, :LANES] + carry)
        carry = carry + both[:, LANES:]
    return jnp.concatenate(pieces, axis=1).astype(I32)


def write_out(gate_v, up_v, gate_h, up_h, sems):
    copies = [
        pltpu.make_async_copy(src.at[layer, part], dst.at[layer, part], sems.at[4 * n + 2 * layer + part])
        for n, (src, dst) in enumerate(((gate_v, gate_h), (up_v, up_h)))
        for layer in range(2)
        for part in range(2)
    ]
    for copy in copies:
        copy.start()
    for copy in copies:
        copy.wait()


def solution(mesh):
    blocks, splits = mesh.shape["section"], mesh.shape["mp"]
    z_chips = blocks // 4
    reach = z_chips // 4

    def steps(first, last):
        order = [d for n in range(last, first - 1, -1) for d in ((n, z_chips - n) if 0 < n < z_chips // 2 else (n,))]
        return [(d, q) for d in order for q in range(4) if d or q]

    near = steps(0, reach)
    n_far = z_chips - 2 * reach - 1

    def local(gate_weight, up_weight, hidden_map, ffn_map):
        layers, rows, narrow = gate_weight.shape
        extra = ffn_map.shape[0] // splits
        wide = narrow + extra
        cap = extra // splits
        filled = -(-cap // 32) * 32
        main = narrow // LANES * LANES
        tail = narrow - main
        lead = main + LANES
        padded = -(-extra // LANES) * LANES
        spread = -(-(wide - main) // LANES) * LANES
        hrows = hidden_map.shape[0] // LANES
        frows = ffn_map.shape[0] // LANES
        per_row = LANES // rows
        cols = splits * LANES

        def kernel(gate_h, up_h, hmap_h, fmap_h, out_g, out_u, gv, uv, hm, fm, own1, own0, send1, recv1, send0, recv0,
                   got, fr, colpick, place, bsend, brecv, in_sem, s1, r1, s0, r0, sb, rb, ready):
            outs = (out_g, out_u)
            me = lax.axis_index("section")
            col = lax.axis_index("mp")
            half, z, core = me // (2 * z_chips), (me // 2) % z_chips, me % 2
            ring = [2 * z] + [2 * jnp.where(z + d >= z_chips, z + d - z_chips, z + d) for d in range(1, z_chips)]
            seat = [h * (2 * z_chips) + c for h in (half, 1 - half) for c in (core, 1 - core)]
            fellow = [jnp.where(col + k >= splits, col + k - splits, col + k) for k in range(splits)]

            barrier = pltpu.get_barrier_semaphore()
            for d, q in near:
                pl.semaphore_signal(barrier, 1, device_id={"section": seat[q] + ring[d]}, device_id_type=MESH)
            for to in fellow[1:]:
                pl.semaphore_signal(barrier, 1, device_id={"mp": to}, device_id_type=MESH)

            loads = [
                pltpu.make_async_copy(src, dst, in_sem.at[n])
                for n, (src, dst) in enumerate(((hmap_h, hm), (gate_h, gv), (up_h, uv), (fmap_h, fm)))
            ]
            for copy in loads:
                copy.start()

            loads[0].wait()
            spread_map = jnp.concatenate([jnp.broadcast_to(hm[r : r + 1, :], (2 * per_row, LANES)) for r in range(hrows)], axis=0)
            shape = (2 * blocks, LANES)
            within = spread_map - me * rows
            mine = (within >= 0) & (within < rows) & (lane_iota(shape) // rows == (row_iota(shape) // 2) % per_row)
            chosen = jnp.sum(jnp.where(mine, within + 1, 0), axis=1, keepdims=True) - 1
            side = row_iota((2 * blocks, 1)) % 2
            target = jnp.where(chosen >= 0, chosen + side * rows, -1)
            pick_rows = one_hot(target == lane_iota((2 * blocks, 2 * rows)))

            used = jnp.zeros((rows, LANES), F32)
            for r in range(hrows):
                entry = jnp.broadcast_to(hm[r : r + 1, :], (rows, LANES))
                used = used + (entry == me * rows + row_iota((rows, LANES))).astype(F32)
            counts = jnp.sum(used, axis=1, keepdims=True) + 1.0
            counts = jnp.concatenate([counts, counts], axis=0)

            loads[1].wait()
            loads[2].wait()
            new = [(jnp.concatenate([gv[layer], uv[layer]], axis=0).astype(F32) / counts) for layer in range(2)]
            own1[:, :main] = new[1][:, :main].astype(BF16)
            own1[:, main:] = jnp.concatenate([new[1][:, main:], new[0][:, main:]], axis=1).astype(BF16)
            own0[...] = new[0][:, :main].astype(BF16)
            send1[...] = jnp.dot(pick_rows, own1[...], preferred_element_type=F32).astype(BF16).reshape(send1.shape)
            send0[...] = jnp.dot(pick_rows, own0[...], preferred_element_type=F32).astype(BF16).reshape(send0.shape)
            recv1[me] = send1[me]
            recv0[me] = send0[me]

            pl.semaphore_wait(barrier, len(near) + splits - 1)
            for d in (reach, z_chips - reach):
                pl.semaphore_signal(ready, 1, device_id={"section": seat[0] + ring[d]}, device_id_type=MESH)

            def send(layer, to):
                src, dst, ss, rs = ((send0, recv0, s0, r0), (send1, recv1, s1, r1))[layer]
                pltpu.make_async_remote_copy(
                    src.at[to], dst.at[me], ss, rs, device_id={"section": to}, device_id_type=MESH
                ).start()

            for d, q in near:
                send(1, seat[q] + ring[d])

            loads[3].wait()
            for m in range(splits):
                first, shift = m * extra // LANES, m * extra % LANES
                n_rows = min(padded // LANES + 1, frows - first)
                flat = jnp.concatenate([fm[first + r : first + r + 1, :] for r in range(n_rows)], axis=1)
                fr[m : m + 1, :extra] = flat[:, shift : shift + extra]
            fr[:, extra:] = jnp.full((splits, padded - extra), -1, I32)

            within = fr[...] - col * narrow
            hit = (within >= 0) & (within < narrow)
            rank = jnp.where(hit, ranks(hit, padded), -1)
            for m in range(splits):
                taken = rank[m : m + 1, :] == row_iota((filled, padded))
                column = jnp.sum(jnp.where(taken, within[m : m + 1, :] + 1, 0), axis=1, keepdims=True) - 1
                colpick[m * LANES : m * LANES + filled, :] = one_hot(column == lane_iota((filled, narrow)))
                colpick[m * LANES + filled : (m + 1) * LANES, :] = jnp.zeros((LANES - filled, narrow), BF16)

            def exchange(part, values):
                def choose(to):
                    picks = colpick[pl.ds(pl.multiple_of(to * LANES, LANES), LANES), :]
                    chosen = lax.dot_general(values, picks, (((1,), (1,)), ((), ())), preferred_element_type=F32)
                    bsend[part, to] = chosen.astype(BF16)

                for k in sorted(range(1, splits), key=lambda k: -min(k % 4, 4 - k % 4)):
                    to = fellow[k]
                    choose(to)
                    pltpu.make_async_remote_copy(
                        bsend.at[part, to], brecv.at[part, col], sb.at[part], rb.at[part], device_id={"mp": to}, device_id_type=MESH
                    ).start()
                choose(col)
                brecv[part, col] = bsend[part, col]

            def arrived(buffers, sem):
                src, dst = buffers
                pltpu.make_async_copy(src.at[pl.ds(0, dst.shape[0] - 1)], dst.at[pl.ds(0, dst.shape[0] - 1)], sem).wait()

            def grow(part, last):
                arrived((bsend.at[part], brecv.at[part]), rb.at[part])
                added = jnp.zeros((2 * rows, spread), F32)
                for m in range(splits):
                    added += jnp.dot(brecv[part, m], place[m * LANES : (m + 1) * LANES, :], preferred_element_type=F32)
                first_half = lane_iota((2 * rows, LANES)) < tail
                for layer, end in enumerate((pltpu.roll(last, LANES - tail, 1), last)):
                    head = (added[:, :LANES] + jnp.where(first_half, end, 0.0)).astype(BF16)
                    for w in range(2):
                        a, b = w * rows, (w + 1) * rows
                        outs[w][layer, part, :, main:lead] = head[a:b, :]
                        outs[w][layer, part, :, lead:] = added[a:b, LANES : wide - main].astype(BF16)

            exchange(0, own1[:, :narrow])

            pl.semaphore_wait(ready, 2)
            turned = jnp.where((z + reach + 1 < z_chips) & (z + reach + n_far >= z_chips), z_chips - 1 - reach - z, 0)
            for i in range(n_far):
                ahead = jnp.where(i + turned >= n_far, i + turned - n_far, i + turned) + reach + 1 + z
                for q in range(4):
                    send(1, seat[q] + 2 * jnp.where(ahead >= z_chips, ahead - z_chips, ahead))

            wanted = jnp.broadcast_to(fr[pl.ds(col, 1), :], (splits, padded)) - row_iota((splits, padded)) * narrow
            hit = (wanted >= 0) & (wanted < narrow)
            code = jnp.where(hit, ranks(hit, padded) + row_iota((splits, padded)) * LANES + 1, 0)
            code = jnp.sum(code, axis=0, keepdims=True) - 1
            code = jnp.concatenate([jnp.full((1, tail), -1, I32), code[:, : spread - tail]], axis=1)
            place[...] = one_hot(code == row_iota((cols, spread)))

            entry = jnp.broadcast_to(hm[pl.ds(me // per_row, 1), :], (rows, LANES))
            place_of = lane_iota((rows, LANES)) == (me % per_row) * rows + row_iota((rows, LANES))
            owner = jnp.sum(jnp.where(place_of, entry, 0), axis=1, keepdims=True) // rows
            landing = jnp.concatenate([2 * owner, 2 * owner + 1], axis=0)
            arrive = one_hot(landing == lane_iota((2 * rows, 2 * blocks)))

            for w in range(2):
                a, b = w * rows, (w + 1) * rows
                outs[w][0, 0, :, :main] = own0[a:b, :]
                outs[w][1, 0, :, :main] = own1[a:b, :main]
            arrived((send1, recv1), s1)
            for j in range(z_chips):
                for q in range(1, 4):
                    send(0, seat[q] + 2 * j)
                pl.when(z != j)(functools.partial(send, 0, seat[0] + 2 * j))
            grow(0, own1[:, main:].astype(F32))

            arrived((send1, recv1), r1)
            got[...] = jnp.dot(arrive, recv1[...].reshape(2 * blocks, lead), preferred_element_type=F32).astype(BF16)
            exchange(1, got[:, :narrow])
            for w in range(2):
                outs[w][1, 1, :, :main] = got[w * rows : (w + 1) * rows, :main]
            arrived((send0, recv0), r0)
            got0 = jnp.dot(arrive, recv0[...].reshape(2 * blocks, main), preferred_element_type=F32).astype(BF16)
            for w in range(2):
                outs[w][0, 1, :, :main] = got0[w * rows : (w + 1) * rows, :]
            grow(1, got[:, main:].astype(F32))

            arrived((send0, recv0), s0)
            for part in range(2):
                arrived((bsend.at[part], brecv.at[part]), sb.at[part])

        out = jax.ShapeDtypeStruct((layers, 2, rows, wide), BF16)
        anywhere = pl.BlockSpec(memory_space=pl.ANY)
        inside = pl.BlockSpec(memory_space=pltpu.VMEM)
        both = (out, out)
        operands = (gate_weight, up_weight, hidden_map.reshape(hrows, LANES), ffn_map.reshape(frows, LANES))
        grown = pl.pallas_call(
            kernel,
            out_shape=both,
            in_specs=[pl.BlockSpec(memory_space=pltpu.HBM)] * 4,
            out_specs=(inside, inside),
            scratch_shapes=[
                pltpu.VMEM(gate_weight.shape, BF16),
                pltpu.VMEM(gate_weight.shape, BF16),
                pltpu.VMEM((hrows, LANES), I32),
                pltpu.VMEM((frows, LANES), I32),
                pltpu.VMEM((2 * rows, lead), BF16),
                pltpu.VMEM((2 * rows, main), BF16),
                pltpu.VMEM((blocks, 2, lead), BF16),
                pltpu.VMEM((blocks, 2, lead), BF16),
                pltpu.VMEM((blocks, 2, main), BF16),
                pltpu.VMEM((blocks, 2, main), BF16),
                pltpu.VMEM((2 * rows, lead), BF16),
                pltpu.VMEM((splits, padded), I32),
                pltpu.VMEM((cols, narrow), BF16),
                pltpu.VMEM((cols, spread), BF16),
                pltpu.VMEM((2, splits, 2 * rows, LANES), BF16),
                pltpu.VMEM((2, splits, 2 * rows, LANES), BF16),
                pltpu.SemaphoreType.DMA((4,)),
                pltpu.SemaphoreType.DMA,
                pltpu.SemaphoreType.DMA,
                pltpu.SemaphoreType.DMA,
                pltpu.SemaphoreType.DMA,
                pltpu.SemaphoreType.DMA((2,)),
                pltpu.SemaphoreType.DMA((2,)),
                pltpu.SemaphoreType.REGULAR,
            ],
            compiler_params=pltpu.CompilerParams(collective_id=0, has_side_effects=True, vmem_limit_bytes=24 << 20),
            name="grow",
        )(*(pltpu.with_memory_space_constraint(x, pltpu.HBM) for x in operands))
        return pl.pallas_call(
            write_out,
            out_shape=both,
            in_specs=[inside] * 2,
            out_specs=(anywhere, anywhere),
            scratch_shapes=[pltpu.SemaphoreType.DMA((8,))],
            compiler_params=pltpu.CompilerParams(vmem_limit_bytes=24 << 20),
            name="write",
        )(*grown)

    weights = P(None, "section", "mp")
    out_specs = (P(None, None, "section", "mp"),) * 2
    return jax.shard_map(local, mesh=mesh, in_specs=(weights, weights, P(), P()), out_specs=out_specs, check_vma=False)
```

```python
import functools

import jax
import jax.numpy as jnp
from jax import lax
from jax.experimental import pallas as pl
from jax.experimental.pallas import tpu as pltpu
from jax.sharding import PartitionSpec as P

MESH = pl.DeviceIdType.MESH
BF16, F32, I32 = jnp.bfloat16, jnp.float32, jnp.int32
LANES = 128


def lane_iota(shape):
    return lax.broadcasted_iota(I32, shape, len(shape) - 1)


def row_iota(shape):
    return lax.broadcasted_iota(I32, shape, len(shape) - 2)


def one_hot(hit):
    return hit.astype(F32).astype(BF16)


def ranks(hit, wide):
    upper = row_iota((LANES, LANES)) < lane_iota((LANES, LANES))
    steps = jnp.concatenate([upper.astype(F32), jnp.ones((LANES, LANES), F32)], axis=1).astype(BF16)
    flags = one_hot(hit)
    carry = jnp.zeros((hit.shape[0], LANES), F32)
    pieces = []
    for t in range(wide // LANES):
        both = jnp.dot(flags[:, t * LANES : (t + 1) * LANES], steps, preferred_element_type=F32)
        pieces.append(both[:, :LANES] + carry)
        carry = carry + both[:, LANES:]
    return jnp.concatenate(pieces, axis=1).astype(I32)


def write_out(gate_v, up_v, gate_h, up_h, sems):
    copies = [
        pltpu.make_async_copy(src.at[layer, part], dst.at[layer, part], sems.at[4 * n + 2 * layer + part])
        for n, (src, dst) in enumerate(((gate_v, gate_h), (up_v, up_h)))
        for layer in range(2)
        for part in range(2)
    ]
    for copy in copies:
        copy.start()
    for copy in copies:
        copy.wait()


def solution(mesh):
    blocks, splits = mesh.shape["section"], mesh.shape["mp"]
    z_chips = blocks // 4
    reach = z_chips // 4

    def steps(first, last):
        order = [d for n in range(last, first - 1, -1) for d in ((n, z_chips - n) if 0 < n < z_chips // 2 else (n,))]
        return [(d, q) for d in order for q in range(4) if d or q]

    near = steps(0, reach)
    n_far = z_chips - 2 * reach - 1

    def local(gate_weight, up_weight, hidden_map, ffn_map):
        layers, rows, narrow = gate_weight.shape
        extra = ffn_map.shape[0] // splits
        wide = narrow + extra
        cap = extra // splits
        filled = -(-cap // 32) * 32
        main = narrow // LANES * LANES
        tail = narrow - main
        lead = main + LANES
        padded = -(-extra // LANES) * LANES
        spread = -(-(wide - main) // LANES) * LANES
        hrows = hidden_map.shape[0] // LANES
        frows = ffn_map.shape[0] // LANES
        per_row = LANES // rows
        cols = splits * LANES

        def kernel(gate_h, up_h, hmap_h, fmap_h, out_g, out_u, gv, uv, hm, fm, own1, own0, send1, recv1, send0, recv0,
                   got, fr, colpick, place, bsend, brecv, in_sem, s1, r1, s0, r0, sb, rb, ready):
            outs = (out_g, out_u)
            me = lax.axis_index("section")
            col = lax.axis_index("mp")
            half, z, core = me // (2 * z_chips), (me // 2) % z_chips, me % 2
            ring = [2 * z] + [2 * jnp.where(z + d >= z_chips, z + d - z_chips, z + d) for d in range(1, z_chips)]
            seat = [h * (2 * z_chips) + c for h in (half, 1 - half) for c in (core, 1 - core)]
            fellow = [jnp.where(col + k >= splits, col + k - splits, col + k) for k in range(splits)]

            barrier = pltpu.get_barrier_semaphore()
            for d, q in sorted(near, key=lambda s: -(min(s[0], z_chips - s[0]) + 2 * (s[1] // 2))):
                pl.semaphore_signal(barrier, 1, device_id={"section": seat[q] + ring[d]}, device_id_type=MESH)
            for to in fellow[1:]:
                pl.semaphore_signal(barrier, 1, device_id={"mp": to}, device_id_type=MESH)

            loads = [
                pltpu.make_async_copy(src, dst, in_sem.at[n])
                for n, (src, dst) in enumerate(((hmap_h, hm), (gate_h, gv), (up_h, uv), (fmap_h, fm)))
            ]
            for copy in loads:
                copy.start()

            loads[0].wait()
            spread_map = jnp.concatenate([jnp.broadcast_to(hm[r : r + 1, :], (2 * per_row, LANES)) for r in range(hrows)], axis=0)
            shape = (2 * blocks, LANES)
            within = spread_map - me * rows
            mine = (within >= 0) & (within < rows) & (lane_iota(shape) // rows == (row_iota(shape) // 2) % per_row)
            chosen = jnp.sum(jnp.where(mine, within + 1, 0), axis=1, keepdims=True) - 1
            side = row_iota((2 * blocks, 1)) % 2
            target = jnp.where(chosen >= 0, chosen + side * rows, -1)
            pick_rows = one_hot(target == lane_iota((2 * blocks, 2 * rows)))

            used = jnp.zeros((rows, LANES), F32)
            for r in range(hrows):
                entry = jnp.broadcast_to(hm[r : r + 1, :], (rows, LANES))
                used = used + (entry == me * rows + row_iota((rows, LANES))).astype(F32)
            counts = jnp.sum(used, axis=1, keepdims=True) + 1.0
            counts = jnp.concatenate([counts, counts], axis=0)

            loads[1].wait()
            loads[2].wait()
            new = [(jnp.concatenate([gv[layer], uv[layer]], axis=0).astype(F32) / counts) for layer in range(2)]
            own1[:, :main] = new[1][:, :main].astype(BF16)
            own1[:, main:] = jnp.concatenate([new[1][:, main:], new[0][:, main:]], axis=1).astype(BF16)
            own0[...] = new[0][:, :main].astype(BF16)
            send1[...] = jnp.dot(pick_rows, own1[...], preferred_element_type=F32).astype(BF16).reshape(send1.shape)
            send0[...] = jnp.dot(pick_rows, own0[...], preferred_element_type=F32).astype(BF16).reshape(send0.shape)
            recv1[me] = send1[me]
            recv0[me] = send0[me]

            pl.semaphore_wait(barrier, len(near) + splits - 1)
            for d in (reach, z_chips - reach):
                pl.semaphore_signal(ready, 1, device_id={"section": seat[0] + ring[d]}, device_id_type=MESH)

            def send(layer, to):
                src, dst, ss, rs = ((send0, recv0, s0, r0), (send1, recv1, s1, r1))[layer]
                pltpu.make_async_remote_copy(
                    src.at[to], dst.at[me], ss, rs, device_id={"section": to}, device_id_type=MESH
                ).start()

            n_near = 2 * reach + 1
            turned = jnp.where(z < reach, reach - z, jnp.where(z >= z_chips - reach, z_chips + reach - z, 0))
            for i in range(n_near):
                e = jnp.where(i + turned >= n_near, i + turned - n_near, i + turned)
                ahead = z - reach + e
                ahead = jnp.where(ahead < 0, ahead + z_chips, jnp.where(ahead >= z_chips, ahead - z_chips, ahead))
                for q in range(1, 4):
                    send(1, seat[q] + 2 * ahead)
                pl.when(e != reach)(functools.partial(send, 1, seat[0] + 2 * ahead))

            loads[3].wait()
            for m in range(splits):
                first, shift = m * extra // LANES, m * extra % LANES
                n_rows = min(padded // LANES + 1, frows - first)
                flat = jnp.concatenate([fm[first + r : first + r + 1, :] for r in range(n_rows)], axis=1)
                fr[m : m + 1, :extra] = flat[:, shift : shift + extra]
            fr[:, extra:] = jnp.full((splits, padded - extra), -1, I32)

            within = fr[...] - col * narrow
            hit = (within >= 0) & (within < narrow)
            rank = jnp.where(hit, ranks(hit, padded), -1)
            for m in range(splits):
                taken = rank[m : m + 1, :] == row_iota((filled, padded))
                column = jnp.sum(jnp.where(taken, within[m : m + 1, :] + 1, 0), axis=1, keepdims=True) - 1
                colpick[m * LANES : m * LANES + filled, :] = one_hot(column == lane_iota((filled, narrow)))
                colpick[m * LANES + filled : (m + 1) * LANES, :] = jnp.zeros((LANES - filled, narrow), BF16)

            def exchange(part, values):
                def choose(to):
                    picks = colpick[pl.ds(pl.multiple_of(to * LANES, LANES), LANES), :]
                    chosen = lax.dot_general(values, picks, (((1,), (1,)), ((), ())), preferred_element_type=F32)
                    bsend[part, to] = chosen.astype(BF16)

                for k in sorted(range(1, splits), key=lambda k: -min(k % 4, 4 - k % 4)):
                    to = fellow[k]
                    choose(to)
                    pltpu.make_async_remote_copy(
                        bsend.at[part, to], brecv.at[part, col], sb.at[part], rb.at[part], device_id={"mp": to}, device_id_type=MESH
                    ).start()
                choose(col)
                brecv[part, col] = bsend[part, col]

            def arrived(buffers, sem):
                src, dst = buffers
                pltpu.make_async_copy(src.at[pl.ds(0, dst.shape[0] - 1)], dst.at[pl.ds(0, dst.shape[0] - 1)], sem).wait()

            def grow(part, last):
                arrived((bsend.at[part], brecv.at[part]), rb.at[part])
                added = jnp.zeros((2 * rows, spread), F32)
                for m in range(splits):
                    added += jnp.dot(brecv[part, m], place[m * LANES : (m + 1) * LANES, :], preferred_element_type=F32)
                first_half = lane_iota((2 * rows, LANES)) < tail
                for layer, end in enumerate((pltpu.roll(last, LANES - tail, 1), last)):
                    head = (added[:, :LANES] + jnp.where(first_half, end, 0.0)).astype(BF16)
                    for w in range(2):
                        a, b = w * rows, (w + 1) * rows
                        outs[w][layer, part, :, main:lead] = head[a:b, :]
                        outs[w][layer, part, :, lead:] = added[a:b, LANES : wide - main].astype(BF16)

            exchange(0, own1[:, :narrow])

            pl.semaphore_wait(ready, 2)
            turned = jnp.where((z + reach + 1 < z_chips) & (z + reach + n_far >= z_chips), z_chips - 1 - reach - z, 0)
            for i in range(n_far):
                ahead = jnp.where(i + turned >= n_far, i + turned - n_far, i + turned) + reach + 1 + z
                for q in range(4):
                    send(1, seat[q] + 2 * jnp.where(ahead >= z_chips, ahead - z_chips, ahead))

            wanted = jnp.broadcast_to(fr[pl.ds(col, 1), :], (splits, padded)) - row_iota((splits, padded)) * narrow
            hit = (wanted >= 0) & (wanted < narrow)
            code = jnp.where(hit, ranks(hit, padded) + row_iota((splits, padded)) * LANES + 1, 0)
            code = jnp.sum(code, axis=0, keepdims=True) - 1
            code = jnp.concatenate([jnp.full((1, tail), -1, I32), code[:, : spread - tail]], axis=1)
            place[...] = one_hot(code == row_iota((cols, spread)))

            entry = jnp.broadcast_to(hm[pl.ds(me // per_row, 1), :], (rows, LANES))
            place_of = lane_iota((rows, LANES)) == (me % per_row) * rows + row_iota((rows, LANES))
            owner = jnp.sum(jnp.where(place_of, entry, 0), axis=1, keepdims=True) // rows
            landing = jnp.concatenate([2 * owner, 2 * owner + 1], axis=0)
            arrive = one_hot(landing == lane_iota((2 * rows, 2 * blocks)))

            for w in range(2):
                a, b = w * rows, (w + 1) * rows
                outs[w][0, 0, :, :main] = own0[a:b, :]
                outs[w][1, 0, :, :main] = own1[a:b, :main]
            arrived((send1, recv1), s1)
            for j in range(z_chips):
                for q in range(1, 4):
                    send(0, seat[q] + 2 * j)
                pl.when(z != j)(functools.partial(send, 0, seat[0] + 2 * j))
            grow(0, own1[:, main:].astype(F32))

            arrived((send1, recv1), r1)
            got[...] = jnp.dot(arrive, recv1[...].reshape(2 * blocks, lead), preferred_element_type=F32).astype(BF16)
            exchange(1, got[:, :narrow])
            for w in range(2):
                outs[w][1, 1, :, :main] = got[w * rows : (w + 1) * rows, :main]
            arrived((send0, recv0), r0)
            got0 = jnp.dot(arrive, recv0[...].reshape(2 * blocks, main), preferred_element_type=F32).astype(BF16)
            for w in range(2):
                outs[w][0, 1, :, :main] = got0[w * rows : (w + 1) * rows, :]
            grow(1, got[:, main:].astype(F32))

            arrived((send0, recv0), s0)
            for part in range(2):
                arrived((bsend.at[part], brecv.at[part]), sb.at[part])

        out = jax.ShapeDtypeStruct((layers, 2, rows, wide), BF16)
        anywhere = pl.BlockSpec(memory_space=pl.ANY)
        inside = pl.BlockSpec(memory_space=pltpu.VMEM)
        both = (out, out)
        operands = (gate_weight, up_weight, hidden_map.reshape(hrows, LANES), ffn_map.reshape(frows, LANES))
        grown = pl.pallas_call(
            kernel,
            out_shape=both,
            in_specs=[pl.BlockSpec(memory_space=pltpu.HBM)] * 4,
            out_specs=(inside, inside),
            scratch_shapes=[
                pltpu.VMEM(gate_weight.shape, BF16),
                pltpu.VMEM(gate_weight.shape, BF16),
                pltpu.VMEM((hrows, LANES), I32),
                pltpu.VMEM((frows, LANES), I32),
                pltpu.VMEM((2 * rows, lead), BF16),
                pltpu.VMEM((2 * rows, main), BF16),
                pltpu.VMEM((blocks, 2, lead), BF16),
                pltpu.VMEM((blocks, 2, lead), BF16),
                pltpu.VMEM((blocks, 2, main), BF16),
                pltpu.VMEM((blocks, 2, main), BF16),
                pltpu.VMEM((2 * rows, lead), BF16),
                pltpu.VMEM((splits, padded), I32),
                pltpu.VMEM((cols, narrow), BF16),
                pltpu.VMEM((cols, spread), BF16),
                pltpu.VMEM((2, splits, 2 * rows, LANES), BF16),
                pltpu.VMEM((2, splits, 2 * rows, LANES), BF16),
                pltpu.SemaphoreType.DMA((4,)),
                pltpu.SemaphoreType.DMA,
                pltpu.SemaphoreType.DMA,
                pltpu.SemaphoreType.DMA,
                pltpu.SemaphoreType.DMA,
                pltpu.SemaphoreType.DMA((2,)),
                pltpu.SemaphoreType.DMA((2,)),
                pltpu.SemaphoreType.REGULAR,
            ],
            compiler_params=pltpu.CompilerParams(collective_id=0, has_side_effects=True, vmem_limit_bytes=24 << 20),
            name="grow",
        )(*(pltpu.with_memory_space_constraint(x, pltpu.HBM) for x in operands))
        return pl.pallas_call(
            write_out,
            out_shape=both,
            in_specs=[inside] * 2,
            out_specs=(anywhere, anywhere),
            scratch_shapes=[pltpu.SemaphoreType.DMA((8,))],
            compiler_params=pltpu.CompilerParams(vmem_limit_bytes=24 << 20),
            name="write",
        )(*grown)

    weights = P(None, "section", "mp")
    out_specs = (P(None, None, "section", "mp"),) * 2
    return jax.shard_map(local, mesh=mesh, in_specs=(weights, weights, P(), P()), out_specs=out_specs, check_vma=False)
```

```python
import functools

import jax
import jax.numpy as jnp
from jax import lax
from jax.experimental import pallas as pl
from jax.experimental.pallas import tpu as pltpu
from jax.sharding import PartitionSpec as P

MESH = pl.DeviceIdType.MESH
BF16, F32, I32 = jnp.bfloat16, jnp.float32, jnp.int32
LANES = 128


def lane_iota(shape):
    return lax.broadcasted_iota(I32, shape, len(shape) - 1)


def row_iota(shape):
    return lax.broadcasted_iota(I32, shape, len(shape) - 2)


def one_hot(hit):
    return hit.astype(F32).astype(BF16)


def ranks(hit, wide):
    upper = row_iota((LANES, LANES)) < lane_iota((LANES, LANES))
    steps = jnp.concatenate([upper.astype(F32), jnp.ones((LANES, LANES), F32)], axis=1).astype(BF16)
    flags = one_hot(hit)
    carry = jnp.zeros((hit.shape[0], LANES), F32)
    pieces = []
    for t in range(wide // LANES):
        both = jnp.dot(flags[:, t * LANES : (t + 1) * LANES], steps, preferred_element_type=F32)
        pieces.append(both[:, :LANES] + carry)
        carry = carry + both[:, LANES:]
    return jnp.concatenate(pieces, axis=1).astype(I32)


def write_out(gate_v, up_v, gate_h, up_h, sems):
    copies = [
        pltpu.make_async_copy(src.at[layer, part], dst.at[layer, part], sems.at[4 * n + 2 * layer + part])
        for n, (src, dst) in enumerate(((gate_v, gate_h), (up_v, up_h)))
        for layer in range(2)
        for part in range(2)
    ]
    for copy in copies:
        copy.start()
    for copy in copies:
        copy.wait()


def solution(mesh):
    blocks, splits = mesh.shape["section"], mesh.shape["mp"]
    z_chips = blocks // 4
    reach = z_chips // 4

    def steps(first, last):
        order = [d for n in range(last, first - 1, -1) for d in ((n, z_chips - n) if 0 < n < z_chips // 2 else (n,))]
        return [(d, q) for d in order for q in range(4) if d or q]

    near = steps(0, reach)
    n_far = z_chips - 2 * reach - 1

    def local(gate_weight, up_weight, hidden_map, ffn_map):
        layers, rows, narrow = gate_weight.shape
        extra = ffn_map.shape[0] // splits
        wide = narrow + extra
        cap = extra // splits
        filled = -(-cap // 32) * 32
        main = narrow // LANES * LANES
        tail = narrow - main
        lead = main + LANES
        padded = -(-extra // LANES) * LANES
        spread = -(-(wide - main) // LANES) * LANES
        hrows = hidden_map.shape[0] // LANES
        frows = ffn_map.shape[0] // LANES
        per_row = LANES // rows
        cols = splits * LANES

        def kernel(gate_h, up_h, hmap_h, fmap_h, out_g, out_u, gv, uv, hm, fm, own1, own0, send1, recv1, send0, recv0,
                   got, fr, colpick, place, bsend, brecv, in_sem, s1, r1, s0, r0, sb, rb, ready):
            outs = (out_g, out_u)
            me = lax.axis_index("section")
            col = lax.axis_index("mp")
            half, z, core = me // (2 * z_chips), (me // 2) % z_chips, me % 2
            ring = [2 * z] + [2 * jnp.where(z + d >= z_chips, z + d - z_chips, z + d) for d in range(1, z_chips)]
            seat = [h * (2 * z_chips) + c for h in (half, 1 - half) for c in (core, 1 - core)]
            fellow = [jnp.where(col + k >= splits, col + k - splits, col + k) for k in range(splits)]

            barrier = pltpu.get_barrier_semaphore()
            for d, q in near:
                pl.semaphore_signal(barrier, 1, device_id={"section": seat[q] + ring[d]}, device_id_type=MESH)
            for to in fellow[1:]:
                pl.semaphore_signal(barrier, 1, device_id={"mp": to}, device_id_type=MESH)

            loads = [
                pltpu.make_async_copy(src, dst, in_sem.at[n])
                for n, (src, dst) in enumerate(((hmap_h, hm), (gate_h, gv), (up_h, uv), (fmap_h, fm)))
            ]
            for copy in loads:
                copy.start()

            loads[0].wait()
            spread_map = jnp.concatenate([jnp.broadcast_to(hm[r : r + 1, :], (2 * per_row, LANES)) for r in range(hrows)], axis=0)
            shape = (2 * blocks, LANES)
            within = spread_map - me * rows
            mine = (within >= 0) & (within < rows) & (lane_iota(shape) // rows == (row_iota(shape) // 2) % per_row)
            chosen = jnp.sum(jnp.where(mine, within + 1, 0), axis=1, keepdims=True) - 1
            side = row_iota((2 * blocks, 1)) % 2
            target = jnp.where(chosen >= 0, chosen + side * rows, -1)
            pick_rows = one_hot(target == lane_iota((2 * blocks, 2 * rows)))

            used = jnp.zeros((rows, LANES), F32)
            for r in range(hrows):
                entry = jnp.broadcast_to(hm[r : r + 1, :], (rows, LANES))
                used = used + (entry == me * rows + row_iota((rows, LANES))).astype(F32)
            counts = jnp.sum(used, axis=1, keepdims=True) + 1.0
            counts = jnp.concatenate([counts, counts], axis=0)

            loads[1].wait()
            loads[2].wait()
            new = [(jnp.concatenate([gv[layer], uv[layer]], axis=0).astype(F32) / counts) for layer in range(2)]
            own1[:, :main] = new[1][:, :main].astype(BF16)
            own1[:, main:] = jnp.concatenate([new[1][:, main:], new[0][:, main:]], axis=1).astype(BF16)
            own0[...] = new[0][:, :main].astype(BF16)
            send1[...] = jnp.dot(pick_rows, own1[...], preferred_element_type=F32).astype(BF16).reshape(send1.shape)
            send0[...] = jnp.dot(pick_rows, own0[...], preferred_element_type=F32).astype(BF16).reshape(send0.shape)
            recv1[me] = send1[me]
            recv0[me] = send0[me]

            pl.semaphore_wait(barrier, len(near) + splits - 1)
            for d in (reach, z_chips - reach):
                pl.semaphore_signal(ready, 1, device_id={"section": seat[0] + ring[d]}, device_id_type=MESH)

            def send(layer, to):
                src, dst, ss, rs = ((send0, recv0, s0, r0), (send1, recv1, s1, r1))[layer]
                pltpu.make_async_remote_copy(
                    src.at[to], dst.at[me], ss, rs, device_id={"section": to}, device_id_type=MESH
                ).start()

            for d, q in near:
                send(1, seat[q] + ring[d])

            loads[3].wait()
            for m in range(splits):
                first, shift = m * extra // LANES, m * extra % LANES
                n_rows = min(padded // LANES + 1, frows - first)
                flat = jnp.concatenate([fm[first + r : first + r + 1, :] for r in range(n_rows)], axis=1)
                fr[m : m + 1, :extra] = flat[:, shift : shift + extra]
            fr[:, extra:] = jnp.full((splits, padded - extra), -1, I32)

            within = fr[...] - col * narrow
            hit = (within >= 0) & (within < narrow)
            rank = jnp.where(hit, ranks(hit, padded), -1)
            for m in range(splits):
                taken = rank[m : m + 1, :] == row_iota((filled, padded))
                column = jnp.sum(jnp.where(taken, within[m : m + 1, :] + 1, 0), axis=1, keepdims=True) - 1
                colpick[m * LANES : m * LANES + filled, :] = one_hot(column == lane_iota((filled, narrow)))
                colpick[m * LANES + filled : (m + 1) * LANES, :] = jnp.zeros((LANES - filled, narrow), BF16)

            def exchange(part, values):
                def choose(to):
                    picks = colpick[pl.ds(pl.multiple_of(to * LANES, LANES), LANES), :]
                    chosen = lax.dot_general(values, picks, (((1,), (1,)), ((), ())), preferred_element_type=F32)
                    bsend[part, to] = chosen.astype(BF16)

                for k in sorted(range(1, splits), key=lambda k: -min(k % 4, 4 - k % 4)):
                    to = fellow[k]
                    choose(to)
                    pltpu.make_async_remote_copy(
                        bsend.at[part, to], brecv.at[part, col], sb.at[part], rb.at[part, col], device_id={"mp": to}, device_id_type=MESH
                    ).start()
                choose(col)
                brecv[part, col] = bsend[part, col]

            def arrived(buffers, sem):
                src, dst = buffers
                pltpu.make_async_copy(src.at[pl.ds(0, dst.shape[0] - 1)], dst.at[pl.ds(0, dst.shape[0] - 1)], sem).wait()

            def grow(part, last):
                added = jnp.zeros((2 * rows, spread), F32)
                for k in sorted(range(splits), key=lambda k: min(k % 4, 4 - k % 4) + k // 4):
                    m = fellow[k]
                    if k:
                        pltpu.make_async_copy(bsend.at[part, m], brecv.at[part, m], rb.at[part, m]).wait()
                    spots = place[pl.ds(pl.multiple_of(m * LANES, LANES), LANES), :]
                    added += jnp.dot(brecv[part, m], spots, preferred_element_type=F32)
                first_half = lane_iota((2 * rows, LANES)) < tail
                for layer, end in enumerate((pltpu.roll(last, LANES - tail, 1), last)):
                    head = (added[:, :LANES] + jnp.where(first_half, end, 0.0)).astype(BF16)
                    for w in range(2):
                        a, b = w * rows, (w + 1) * rows
                        outs[w][layer, part, :, main:lead] = head[a:b, :]
                        outs[w][layer, part, :, lead:] = added[a:b, LANES : wide - main].astype(BF16)

            exchange(0, own1[:, :narrow])

            pl.semaphore_wait(ready, 2)
            turned = jnp.where((z + reach + 1 < z_chips) & (z + reach + n_far >= z_chips), z_chips - 1 - reach - z, 0)
            for i in range(n_far):
                ahead = jnp.where(i + turned >= n_far, i + turned - n_far, i + turned) + reach + 1 + z
                for q in range(4):
                    send(1, seat[q] + 2 * jnp.where(ahead >= z_chips, ahead - z_chips, ahead))

            wanted = jnp.broadcast_to(fr[pl.ds(col, 1), :], (splits, padded)) - row_iota((splits, padded)) * narrow
            hit = (wanted >= 0) & (wanted < narrow)
            code = jnp.where(hit, ranks(hit, padded) + row_iota((splits, padded)) * LANES + 1, 0)
            code = jnp.sum(code, axis=0, keepdims=True) - 1
            code = jnp.concatenate([jnp.full((1, tail), -1, I32), code[:, : spread - tail]], axis=1)
            place[...] = one_hot(code == row_iota((cols, spread)))

            entry = jnp.broadcast_to(hm[pl.ds(me // per_row, 1), :], (rows, LANES))
            place_of = lane_iota((rows, LANES)) == (me % per_row) * rows + row_iota((rows, LANES))
            owner = jnp.sum(jnp.where(place_of, entry, 0), axis=1, keepdims=True) // rows
            landing = jnp.concatenate([2 * owner, 2 * owner + 1], axis=0)
            arrive = one_hot(landing == lane_iota((2 * rows, 2 * blocks)))

            for w in range(2):
                a, b = w * rows, (w + 1) * rows
                outs[w][0, 0, :, :main] = own0[a:b, :]
                outs[w][1, 0, :, :main] = own1[a:b, :main]
            arrived((send1, recv1), s1)
            for j in range(z_chips):
                for q in range(1, 4):
                    send(0, seat[q] + 2 * j)
                pl.when(z != j)(functools.partial(send, 0, seat[0] + 2 * j))
            grow(0, own1[:, main:].astype(F32))

            arrived((send1, recv1), r1)
            got[...] = jnp.dot(arrive, recv1[...].reshape(2 * blocks, lead), preferred_element_type=F32).astype(BF16)
            exchange(1, got[:, :narrow])
            for w in range(2):
                outs[w][1, 1, :, :main] = got[w * rows : (w + 1) * rows, :main]
            arrived((send0, recv0), r0)
            got0 = jnp.dot(arrive, recv0[...].reshape(2 * blocks, main), preferred_element_type=F32).astype(BF16)
            for w in range(2):
                outs[w][0, 1, :, :main] = got0[w * rows : (w + 1) * rows, :]
            grow(1, got[:, main:].astype(F32))

            arrived((send0, recv0), s0)
            for part in range(2):
                arrived((bsend.at[part], brecv.at[part]), sb.at[part])

        out = jax.ShapeDtypeStruct((layers, 2, rows, wide), BF16)
        anywhere = pl.BlockSpec(memory_space=pl.ANY)
        inside = pl.BlockSpec(memory_space=pltpu.VMEM)
        both = (out, out)
        operands = (gate_weight, up_weight, hidden_map.reshape(hrows, LANES), ffn_map.reshape(frows, LANES))
        grown = pl.pallas_call(
            kernel,
            out_shape=both,
            in_specs=[pl.BlockSpec(memory_space=pltpu.HBM)] * 4,
            out_specs=(inside, inside),
            scratch_shapes=[
                pltpu.VMEM(gate_weight.shape, BF16),
                pltpu.VMEM(gate_weight.shape, BF16),
                pltpu.VMEM((hrows, LANES), I32),
                pltpu.VMEM((frows, LANES), I32),
                pltpu.VMEM((2 * rows, lead), BF16),
                pltpu.VMEM((2 * rows, main), BF16),
                pltpu.VMEM((blocks, 2, lead), BF16),
                pltpu.VMEM((blocks, 2, lead), BF16),
                pltpu.VMEM((blocks, 2, main), BF16),
                pltpu.VMEM((blocks, 2, main), BF16),
                pltpu.VMEM((2 * rows, lead), BF16),
                pltpu.VMEM((splits, padded), I32),
                pltpu.VMEM((cols, narrow), BF16),
                pltpu.VMEM((cols, spread), BF16),
                pltpu.VMEM((2, splits, 2 * rows, LANES), BF16),
                pltpu.VMEM((2, splits, 2 * rows, LANES), BF16),
                pltpu.SemaphoreType.DMA((4,)),
                pltpu.SemaphoreType.DMA,
                pltpu.SemaphoreType.DMA,
                pltpu.SemaphoreType.DMA,
                pltpu.SemaphoreType.DMA,
                pltpu.SemaphoreType.DMA((2,)),
                pltpu.SemaphoreType.DMA((2, splits)),
                pltpu.SemaphoreType.REGULAR,
            ],
            compiler_params=pltpu.CompilerParams(collective_id=0, has_side_effects=True, vmem_limit_bytes=24 << 20),
            name="grow",
        )(*(pltpu.with_memory_space_constraint(x, pltpu.HBM) for x in operands))
        return pl.pallas_call(
            write_out,
            out_shape=both,
            in_specs=[inside] * 2,
            out_specs=(anywhere, anywhere),
            scratch_shapes=[pltpu.SemaphoreType.DMA((8,))],
            compiler_params=pltpu.CompilerParams(vmem_limit_bytes=24 << 20),
            name="write",
        )(*grown)

    weights = P(None, "section", "mp")
    out_specs = (P(None, None, "section", "mp"),) * 2
    return jax.shard_map(local, mesh=mesh, in_specs=(weights, weights, P(), P()), out_specs=out_specs, check_vma=False)
```
